128 devices in a mesh: dom: 16 (over z, y), cls: 8 (over x, core).
Axes of the slice: x: 4, y: 4, z: 4, core: 2. Of those that a mesh axis runs over, the one named last changes fastest.
Arguments:
- images: bfloat16 [16384, 2, 16384], P(('dom', 'cls')), may hold values from -6 to 6
- slices: bfloat16 [128, 4, 2, 16384], P(('dom', 'cls')), may hold values from -6 to 6
- classes: int32 [16384], P(('dom', 'cls')), may hold values from 0 to 127, as said below
- rotations: int32 [16384], P(('dom', 'cls')), may hold values from 0 to 3
- defocus: int32 [16384], P(('dom', 'cls')), may hold values from 8000 to 29999
- groups: int32 [16384], P(('dom', 'cls')), may hold values from 0 to 1023, as said below
Outputs:
- sigma: float32 [1024, 64], P(('dom', 'cls'))
The draws below stay inside these ranges and needn't reach their ends.
Inputs may be any that keep to these rules, and one draw needn't show every extreme that they name: Class c is owned by device c // 1 of dom+cls. In the rows of one device, at most 2 particles have classes of one owner; in every draw one owner gets exactly 2 from the rows of every device. `groups`: group g is owned by device g // 8 of dom+cls. Every group holds at least 8 particles.
All inputs are finite; a program needn't handle non-finite values.
Results may differ from the reference program's by a relative error of at most 0.0003.
Values may be sent and summed in bfloat16 or wider, within the bound.
No kernel may reach another device: no remote copies, remote signals or barrier semaphores. Data moves between devices by JAX's collectives and lax.ppermute only.
A program may use at most 192 MiB of HBM per device.

```python
import math
import jax
import jax.numpy as jnp
from jax import lax

SIDE = 128
PIX = 16384
SHELLS = 64
ROT = 4
CLS_DEV = 1
CLASSES = 128
P_DEV = 128
PARTICLES = 16384
CAP = 2
GROUPS_DEV = 8
GROUPS = 1024


def draw_classes(key, part):
    owner_count = CLASSES // CLS_DEV
    block_count = PARTICLES // P_DEV
    slot_count = owner_count * CAP
    key_popular, key_bias, key_blocks = jax.random.split(jax.random.fold_in(key, 11), 3)
    popular = jax.random.randint(key_popular, (), 0, owner_count)
    owner_bias = jax.random.randint(key_bias, (owner_count,), 0, 4096)

    def one_block(block_index):
        block_key = jax.random.fold_in(key_blocks, block_index)
        key_noise, key_order, key_within = jax.random.split(block_key, 3)
        noise = jax.random.randint(key_noise, (owner_count, CAP), 0, 4096)
        owner_ids = jnp.broadcast_to(jnp.arange(owner_count, dtype=jnp.int32)[:, None], (owner_count, CAP))
        scores = owner_bias[:, None] + noise + jnp.where(owner_ids == popular, 16384, 0)
        distinct = scores.reshape(-1) * slot_count + jnp.arange(slot_count, dtype=jnp.int32)
        chosen_values, picked = lax.top_k(distinct, P_DEV)
        owner_of = picked.astype(jnp.int32) // CAP
        shuffle = jax.random.permutation(key_order, P_DEV)
        owner_of = owner_of[shuffle]
        within = jax.random.randint(key_within, (P_DEV,), 0, CLS_DEV)
        return owner_of * CLS_DEV + within
    return jax.vmap(one_block)(jnp.arange(block_count, dtype=jnp.int32)).reshape(-1).astype(jnp.int32)


def draw_groups(key, part):
    block_count = PARTICLES // P_DEV
    half_rows = P_DEV // 2
    key_random, key_order = jax.random.split(jax.random.fold_in(key, 23), 2)
    device_ids = jnp.arange(block_count, dtype=jnp.int32)[:, None]
    row_ids = jnp.arange(P_DEV, dtype=jnp.int32)[None, :]
    far_owner = (device_ids + block_count // 2) % block_count
    far_group = far_owner * GROUPS_DEV + row_ids % GROUPS_DEV
    random_group = jax.random.randint(key_random, (block_count, P_DEV), 0, GROUPS)
    base = jnp.where(row_ids < half_rows, far_group, random_group)
    order_keys = jax.random.split(key_order, block_count)
    orders = jax.vmap(lambda one_key: jax.random.permutation(one_key, P_DEV))(order_keys)
    mixed = jnp.take_along_axis(base, orders.astype(jnp.int32), axis=1)
    return mixed.reshape(-1).astype(jnp.int32)


def set_ends(array, key, least, high):
    index_at = [jax.random.randint(jax.random.fold_in(key, axis), (), 0, length) for axis, length in enumerate(array.shape)]
    main_axis = array.shape.index(max(array.shape))
    neighbour = index_at[:main_axis] + [(index_at[main_axis] + 1) % array.shape[main_axis]] + index_at[main_axis + 1:]
    return array.at[tuple(index_at)].set(least).at[tuple(neighbour)].set(high)


def shard_levels(rng, extent, pieces, low, top_value):
    loudness, own = 1.0, jax.random.fold_in(rng, 6)
    for dim, shards_of in pieces:
        heights = jnp.exp(jax.random.uniform(jax.random.fold_in(own, dim), (shards_of,), jnp.float32, low / len(pieces), top_value / len(pieces)))
        loudness = loudness * jnp.repeat(heights, extent[dim] // shards_of).reshape([-1 if axis == dim else 1 for axis in range(len(extent))])
    return loudness


def gaussian(stream_key, dims, scale, bound, shards=(), kind=jnp.bfloat16):
    drawn = scale * jax.random.normal(stream_key, dims, jnp.float32)
    if shards:
        drawn = drawn * shard_levels(stream_key, dims, shards, -0.22, 0.18)
    return jnp.clip(drawn, -bound, bound).astype(kind)


def setup_inputs(seed: int = 0) -> dict:
    key_list = jax.random.split(jax.random.key(seed), 7)
    return {
        "images": gaussian(key_list[0], (PARTICLES, 2, PIX), 1.0, 6.0, ((0, 128),)),
        "slices": gaussian(key_list[1], (CLASSES, ROT, 2, PIX), 1.0, 6.0, ((0, 128),)),
        "classes": draw_classes(jax.random.fold_in(key_list[6], 71), 0),
        "rotations": set_ends(jax.random.randint(key_list[3], (PARTICLES,), 0, ROT), jax.random.fold_in(key_list[3], 1), 0, ROT - 1).astype(jnp.int32),
        "defocus": set_ends(jax.random.randint(key_list[4], (PARTICLES,), 8000, 30000), jax.random.fold_in(key_list[4], 1), 8000, 29999).astype(jnp.int32),
        "groups": draw_groups(jax.random.fold_in(key_list[6], 71), 0),
    }


PIXEL_SIZE = 1.5
WAVELENGTH = 0.0197
SPHERICAL = 27000000.0
AMPLITUDE = 0.1

def frequency_grid(side_cells):
    offsets = jnp.arange(side_cells, dtype=jnp.int32)
    signed = jnp.where(offsets < side_cells // 2, offsets, offsets - side_cells)
    return (signed[:, None] * signed[:, None] + signed[None, :] * signed[None, :]).reshape(-1).astype(jnp.int32)

def shell_matrix(radius_sq, shell_count):
    shell_ids = jnp.arange(shell_count, dtype=jnp.int32)
    lower = shell_ids * shell_ids
    upper = (shell_ids + 1) * (shell_ids + 1)
    in_shell = (lower[None, :] <= radius_sq[:, None]) & (radius_sq[:, None] < upper[None, :])
    return in_shell.astype(jnp.float32)

def contrast(defocus, radius_sq, side_cells):
    spatial = radius_sq.astype(jnp.float32) / jnp.float32((side_cells * PIXEL_SIZE) ** 2)
    depth = defocus.astype(jnp.float32)[:, None]
    phase_shift = math.pi * WAVELENGTH * depth * spatial[None, :] - 0.5 * math.pi * SPHERICAL * WAVELENGTH ** 3 * spatial[None, :] * spatial[None, :]
    return -(math.sqrt(1.0 - AMPLITUDE * AMPLITUDE) * jnp.sin(phase_shift) + AMPLITUDE * jnp.cos(phase_shift))

def power_in_shells(images, fetched, ctf, shell_table):
    difference = images.astype(jnp.float32) - ctf[:, None, :] * fetched.astype(jnp.float32)
    pixel_power = lax.optimization_barrier(jnp.sum(difference * difference, axis=1))
    return jnp.dot(pixel_power, shell_table, precision=lax.Precision.HIGHEST, preferred_element_type=jnp.float32)

def reference(images, slices, classes, rotations, defocus, groups):
    radius_sq = frequency_grid(SIDE)
    shell_table = shell_matrix(radius_sq, SHELLS)
    block_rows = math.gcd(PARTICLES, 512)
    block_count = PARTICLES // block_rows

    def per_block(operands):
        image_rows, class_rows, rotation_rows, defocus_rows = operands
        fetched = slices[class_rows, rotation_rows]
        ctf = contrast(defocus_rows, radius_sq, SIDE)
        return power_in_shells(image_rows, fetched, ctf, shell_table)
    shell_power = lax.map(per_block, (images.reshape(block_count, block_rows, 2, PIX), classes.reshape(block_count, block_rows), rotations.reshape(block_count, block_rows), defocus.reshape(block_count, block_rows))).reshape(PARTICLES, SHELLS)
    group_sums = jax.ops.segment_sum(shell_power, groups, num_segments=GROUPS)
    group_counts = jax.ops.segment_sum(jnp.ones((PARTICLES,), jnp.float32), groups, num_segments=GROUPS)
    pixel_counts = lax.optimization_barrier(jnp.sum(shell_table, axis=0))
    return group_sums / (2.0 * group_counts[:, None] * pixel_counts[None, :])
```

```python
import math

import jax
import jax.numpy as jnp
import numpy as np
from jax import lax
from jax.experimental import pallas as pl
from jax.experimental.pallas import tpu as pltpu
from jax.sharding import Mesh
from jax.sharding import PartitionSpec as P


AXES = ("z", "y", "x", "c")
RING = 4
SIDE = 128
SHELLS = 64
ROT = 4
P_DEV = 128
GROUPS_DEV = 8
DEVICES = 128
GROUPS = GROUPS_DEV * DEVICES
CANDIDATES = 2 * P_DEV

PIXEL_SIZE = 1.5
WAVELENGTH = 0.0197
SPHERICAL = 27000000.0
AMPLITUDE = 0.1

ROWS = 2 * SIDE
ROWS_A = 176
ROWS_B = ROWS - ROWS_A
RINGS_A = (("y", "z", "x"), ("x", "y", "z"))
RINGS_B = (("z", "x", "y"), ("z", "x", "y"))

DEPTH = 32
PACK = 4
NOWHERE = 127


def sine_terms():
    turns = np.cos(np.linspace(0, np.pi, 4001)) * 0.5
    turns = turns[np.abs(turns) > 1e-9]
    basis = np.stack([np.abs(turns) * turns ** (2 * k) for k in range(7)], 1)
    target = np.sin(2 * np.pi * turns) / turns * np.abs(turns)
    return [float(c) for c in np.linalg.lstsq(basis, target, rcond=None)[0]]


SINE = sine_terms()


def frequencies():
    offsets = np.arange(SIDE)
    return np.where(offsets < SIDE // 2, offsets, offsets - SIDE)


def tables():
    freq = frequencies()
    radius_sq = (freq[:, None] ** 2 + freq[None, :] ** 2).astype(np.float64)
    spatial = radius_sq / (SIDE * PIXEL_SIZE) ** 2
    rate = 0.5 * WAVELENGTH * spatial
    shift = -0.25 * SPHERICAL * WAVELENGTH**3 * spatial**2 + math.asin(AMPLITUDE) / (2 * math.pi)
    within = np.zeros((SIDE, 128), np.float32)
    for w in range(SIDE // 2 + 1):
        within[:, w] = np.abs(freq) <= w
    reach = np.full((SIDE, 128), NOWHERE, np.int32)
    for a in range(SIDE):
        for s in range(SHELLS):
            left = (s + 1) ** 2 - 1 - int(freq[a]) ** 2
            if left >= 0:
                reach[a, s] = min(math.isqrt(left), SIDE // 2)
    half = SIDE // 2 + 8
    return (
        rate[:half].astype(np.float32),
        shift[:half].astype(np.float32),
        np.concatenate([within, within], 0),
        reach,
    )


def shell_pixels():
    freq = frequencies()
    radius_sq = freq[:, None] ** 2 + freq[None, :] ** 2
    return np.array(
        [((s * s <= radius_sq) & (radius_sq < (s + 1) ** 2)).sum() for s in range(SHELLS)], np.float32
    )


def shell_kernel(
    n_ref, image_at, a_at, b_at, depth_at, own, other, slice_a, slice_b, rate, shift, within, reach,
    out, image, fetched, square, terms, sem,
):
    steps = (n_ref[0] + 2 * PACK - 1) // (2 * PACK)
    total = steps * 2 * PACK

    def slice_copies(j, slot):
        return (
            pltpu.make_async_copy(slice_a.at[a_at[j]], fetched.at[slot, pl.ds(0, ROWS_A)], sem.at[1, slot]),
            pltpu.make_async_copy(slice_b.at[b_at[j]], fetched.at[slot, pl.ds(ROWS_A, ROWS_B)], sem.at[2, slot]),
        )

    def start(j, slot):
        for copy in slice_copies(j, slot):
            copy.start()
        at = image_at[j]

        @pl.when(at < P_DEV)
        def _():
            pltpu.make_async_copy(own.at[at], image.at[slot], sem.at[0, slot]).start()

        @pl.when(at >= P_DEV)
        def _():
            pltpu.make_async_copy(other.at[at - P_DEV], image.at[slot], sem.at[0, slot]).start()

    def wait(j, slot):
        for copy in slice_copies(j, slot):
            copy.wait()
        pltpu.make_async_copy(own.at[0], image.at[slot], sem.at[0, slot]).wait()

    out[...] = jnp.zeros_like(out)
    for j in range(DEPTH):

        @pl.when(j < total)
        def _(j=j):
            start(j, j)

    half = lax.broadcasted_iota(jnp.int32, (8, 128), 0) // 2
    first = half == 0
    low, high, zero, down = half, half + 4, half * 0, 4 - half
    wrap = jnp.where(first, 0, 8 - half)

    def rows_of(v, index):
        return jnp.take_along_axis(v, index, axis=0, mode="promise_in_bounds")

    def waves(j):
        depth = depth_at[j]
        result = []
        for g in range(SIDE // 16 + 1):
            turns = depth * rate[8 * g : 8 * g + 8, :] + shift[8 * g : 8 * g + 8, :]
            turns = turns - jnp.round(turns)
            sq = turns * turns
            y = sq * SINE[-1] + SINE[-2]
            for term in SINE[-3::-1]:
                y = y * sq + term
            result.append(y * turns)
        return result

    def spread(s, v):
        if v < 16:
            return rows_of(s[v // 2], high if v % 2 else low)
        h = v - 16
        if h % 2:
            return rows_of(s[(15 - h) // 2], down)
        m = 8 - h // 2
        return jnp.where(first, rows_of(s[m], zero), rows_of(s[m - 1], wrap))

    def power(j, slot, k, m):
        s = waves(j)
        for g in range(ROWS // 16):
            r = pl.ds(16 * g, 16)
            wave = jnp.concatenate([spread(s, 2 * g), spread(s, 2 * g + 1)], 0)
            e = image[slot, r, :].astype(jnp.float32) + wave * fetched[slot, r, :].astype(jnp.float32)
            square[m % 2, r, :] = e * e
            if g % 2:
                b = g // 2
                p = square[m % 2, pl.ds(32 * b, 16, stride=2), :] + square[m % 2, pl.ds(32 * b + 1, 16, stride=2), :]
                high_part = p.astype(jnp.bfloat16)
                q = pl.ds(SIDE * m + 16 * b, 16)
                terms[k, q, 0:128] = high_part
                terms[k, q, 128:256] = (p - high_part.astype(jnp.float32)).astype(jnp.bfloat16)

    def collect(sums, j, m):
        parts = [jnp.zeros((8, 128), jnp.float32) for _ in range(2)]
        for g in range(SIDE // 8):
            row = sums[SIDE * m + 8 * g : SIDE * m + 8 * g + 8]
            index = reach[8 * g : 8 * g + 8, :]
            parts[g % 2] = parts[g % 2] + jnp.take_along_axis(row, index, axis=1, mode="promise_in_bounds")
        out[pl.ds(j, 1), :] = jnp.sum(parts[0] + parts[1], axis=0, keepdims=True)

    def region(j, slot, k, before):
        sums = jnp.dot(terms[1 - k], within[...], preferred_element_type=jnp.float32)
        for m in range(PACK):
            power(j + m, slot + m, k, m)
            collect(sums, before + m, m)

    def step(i, carry):
        j = 2 * PACK * i
        slot = lax.rem(j, DEPTH)
        for m in range(2 * PACK):
            wait(j + m, slot + m)
        region(j, slot, 0, jnp.maximum(j - PACK, 0))
        region(j + PACK, slot + PACK, 1, j)
        for m in range(2 * PACK):

            @pl.when(j + m + DEPTH < total)
            def _(m=m):
                start(j + m + DEPTH, slot + m)

        return carry

    terms[...] = jnp.zeros_like(terms)
    lax.fori_loop(0, steps, step, 0)

    @pl.when(total > 0)
    def _():
        sums = jnp.dot(terms[1], within[...], preferred_element_type=jnp.float32)
        for m in range(PACK):
            collect(sums, total - PACK + m, m)

    disks = out[...]
    out[...] = disks - pltpu.roll(disks, 1, 1)


def shell_sums(count, image_at, a_at, b_at, depth, own, other, slice_a, slice_b):
    rate, shift, within, reach = tables()
    smem = pl.BlockSpec(memory_space=pltpu.SMEM)
    hbm = pl.BlockSpec(memory_space=pltpu.HBM)
    vmem = pl.BlockSpec(memory_space=pltpu.VMEM)
    return pl.pallas_call(
        shell_kernel,
        out_shape=jax.ShapeDtypeStruct((CANDIDATES, 128), jnp.float32),
        in_specs=[smem] * 5 + [hbm] * 4 + [vmem] * 4,
        out_specs=vmem,
        scratch_shapes=[
            pltpu.VMEM((DEPTH, ROWS, 128), jnp.bfloat16),
            pltpu.VMEM((DEPTH, ROWS, 128), jnp.bfloat16),
            pltpu.VMEM((2, ROWS, 128), jnp.float32),
            pltpu.VMEM((2, SIDE * PACK, 256), jnp.bfloat16),
            pltpu.SemaphoreType.DMA((3, DEPTH)),
        ],
        name="shell_sums",
    )(
        count, image_at, a_at, b_at, depth, own, other, slice_a, slice_b,
        jnp.asarray(rate), jnp.asarray(shift), jnp.asarray(within, jnp.bfloat16), jnp.asarray(reach),
    )


def ring_pairs(rings, step):
    pairs = []
    for source in range(DEVICES):
        at = {"z": source // 32, "y": source // 8 % 4, "x": source // 2 % 4, "c": source % 2}
        to = dict(at)
        ring = rings[at["c"]]
        to[ring] = (at[ring] + step) % RING
        pairs.append((source, ((to["z"] * 4 + to["y"]) * 4 + to["x"]) * 2 + to["c"]))
    return pairs


def gather_ring(x, rings):
    half = x.shape[0] // 2
    up, down = ring_pairs(rings, 1), ring_pairs(rings, -1)
    left = lax.ppermute(x, AXES, up)
    right = lax.ppermute(x, AXES, down)
    far = lax.ppermute(left[:half], AXES, up), lax.ppermute(right[half:], AXES, down)
    return jnp.concatenate([x, right, *far, left], 0)


def gather_slices(x, rings):
    for phase in range(3):
        x = gather_ring(x, (rings[0][phase], rings[1][phase]))
    return x


def place_of(owner, rotation, rings, core):
    here = {a: lax.axis_index(a) for a in AXES}
    ahead = {
        "z": (owner // 32 - here["z"]) % RING,
        "y": (owner // 8 % 4 - here["y"]) % RING,
        "x": (owner // 2 % 4 - here["x"]) % RING,
    }
    places = [((ahead[r[2]] * 4 + ahead[r[1]]) * 4 + ahead[r[0]]) * ROT + rotation for r in rings]
    return jnp.where(core == 0, places[0], places[1])


def by_rows(x):
    lead = x.shape[:-2]
    x = x.reshape(*lead, 2, SIDE, SIDE)
    return jnp.swapaxes(x, -3, -2).reshape(*lead, ROWS, SIDE)


def body(images, slices, classes, rotations, defocus, groups):
    core = lax.axis_index("c")
    swap = [(0, 1), (1, 0)]
    own_slices = by_rows(slices[0])
    slice_a = gather_slices(own_slices[:, :ROWS_A], RINGS_A)
    slice_b = gather_slices(own_slices[:, ROWS_A:], RINGS_B)
    own = by_rows(images)
    other = lax.ppermute(own, "c", swap)
    facts = jnp.stack([classes, rotations, defocus, groups])
    facts = jnp.concatenate([facts, lax.ppermute(facts, "c", swap)], 1)
    owner, rotation, depth, group = facts
    mine = owner % 2 == core
    index = jnp.arange(CANDIDATES, dtype=jnp.int32)
    rank = jnp.sum((mine[None, :] & (index[None, :] < index[:, None])).astype(jnp.int32), axis=1)
    count = jnp.sum(mine.astype(jnp.int32)).reshape(1)
    chosen = (rank[None, :] == index[:, None]) & mine[None, :]
    a_place = place_of(owner, rotation, RINGS_A, core)
    b_place = place_of(owner, rotation, RINGS_B, core)

    def packed(values):
        return jnp.sum(jnp.where(chosen, values[None, :], 0), axis=1)

    depth = packed(depth).astype(jnp.float32)
    group = jnp.where(index < count, packed(group), -1)
    sums = shell_sums(
        count, packed(index), packed(a_place), packed(b_place), depth, own, other, slice_a, slice_b
    )
    lane = jnp.arange(128, dtype=jnp.int32)
    sums = jnp.where(lane < SHELLS, sums, jnp.where(lane == SHELLS, 1.0, 0.0))
    member = (jnp.arange(GROUPS, dtype=jnp.int32)[:, None] == group[None, :]).astype(jnp.float32)
    partial = jnp.dot(member, sums, precision=lax.Precision.HIGHEST, preferred_element_type=jnp.float32)
    arrived = lax.all_to_all(partial.reshape(DEVICES, GROUPS_DEV, 128), AXES, 0, 0, tiled=True)
    own_groups = jnp.sum(arrived, axis=0)
    return own_groups[:, :SHELLS] / (2.0 * own_groups[:, SHELLS : SHELLS + 1] * jnp.asarray(shell_pixels()))


def solution(mesh):
    finer = Mesh(mesh.devices.reshape(4, 4, 4, 2), AXES)
    placed = (
        P(AXES, None, None),
        P(AXES, None, None, None),
        P(AXES),
        P(AXES),
        P(AXES),
        P(AXES),
    )
    return jax.shard_map(body, mesh=finer, in_specs=placed, out_specs=P(AXES, None), check_vma=False)
```

```python
import math

import jax
import jax.numpy as jnp
import numpy as np
from jax import lax
from jax.experimental import pallas as pl
from jax.experimental.pallas import tpu as pltpu
from jax.sharding import Mesh
from jax.sharding import PartitionSpec as P


AXES = ("z", "y", "x", "c")
RING = 4
SIDE = 128
SHELLS = 64
ROT = 4
P_DEV = 128
GROUPS_DEV = 8
DEVICES = 128
GROUPS = GROUPS_DEV * DEVICES
CANDIDATES = 2 * P_DEV

PIXEL_SIZE = 1.5
WAVELENGTH = 0.0197
SPHERICAL = 27000000.0
AMPLITUDE = 0.1

ROWS = 2 * SIDE
ROWS_A = 176
ROWS_B = ROWS - ROWS_A
RINGS_A = (("y", "z", "x"), ("x", "y", "z"))
RINGS_B = (("z", "x", "y"), ("z", "x", "y"))

DEPTH = 32
PACK = 4
STEP = 2 * PACK
PIECES = 5
SPAN = 64
NOWHERE = 127


def sine_terms():
    turns = np.cos(np.linspace(0, np.pi, 4001)) * 0.5
    turns = turns[np.abs(turns) > 1e-9]
    basis = np.stack([np.abs(turns) * turns ** (2 * k) for k in range(7)], 1)
    target = np.sin(2 * np.pi * turns) / turns * np.abs(turns)
    return [float(c) for c in np.linalg.lstsq(basis, target, rcond=None)[0]]


SINE = sine_terms()


def frequencies():
    offsets = np.arange(SIDE)
    return np.where(offsets < SIDE // 2, offsets, offsets - SIDE)


def tables():
    freq = frequencies()
    radius_sq = (freq[:, None] ** 2 + freq[None, :] ** 2).astype(np.float64)
    spatial = radius_sq / (SIDE * PIXEL_SIZE) ** 2
    rate = 0.5 * WAVELENGTH * spatial
    shift = -0.25 * SPHERICAL * WAVELENGTH**3 * spatial**2 + math.asin(AMPLITUDE) / (2 * math.pi)
    within = np.zeros((SIDE, 128), np.float32)
    for w in range(SIDE // 2 + 1):
        within[:, w] = np.abs(freq) <= w
    reach = np.full((SIDE, 128), NOWHERE, np.int32)
    for a in range(SIDE):
        for s in range(SHELLS):
            left = (s + 1) ** 2 - 1 - int(freq[a]) ** 2
            if left >= 0:
                reach[a, s] = min(math.isqrt(left), SIDE // 2)
    half = SIDE // 2 + 8
    return (
        rate[:half].astype(np.float32),
        shift[:half].astype(np.float32),
        np.concatenate([within, within], 0),
        reach,
    )


def shell_pixels():
    freq = frequencies()
    radius_sq = freq[:, None] ** 2 + freq[None, :] ** 2
    return np.array(
        [((s * s <= radius_sq) & (radius_sq < (s + 1) ** 2)).sum() for s in range(SHELLS)], np.float32
    )


def shell_kernel(
    n_ref, image_at, a_list, b_list, a_ends, b_ends, depth_at, own, other, *refs,
):
    slices_a, slices_b = refs[:PIECES], refs[PIECES : 2 * PIECES]
    rate, shift, within, reach, out, image, fetched, square, terms, image_sem, slice_sem = refs[2 * PIECES :]
    steps = n_ref[0] // STEP
    total = n_ref[0]

    def fetch_slices(places, ends, pieces, rows):
        for b, piece in enumerate(pieces):

            def fetch(t, carry, piece=piece):
                j, at = places[t] // SPAN, places[t] % SPAN
                pltpu.make_async_copy(piece.at[at], fetched.at[j, rows], slice_sem.at[j // STEP]).start()
                return carry

            lax.fori_loop(ends[b], ends[b + 1], fetch, 0)

    def start(j, slot):
        at = image_at[j]

        @pl.when(at < P_DEV)
        def _():
            pltpu.make_async_copy(own.at[at], image.at[slot], image_sem.at[slot]).start()

        @pl.when(at >= P_DEV)
        def _():
            pltpu.make_async_copy(other.at[at - P_DEV], image.at[slot], image_sem.at[slot]).start()

    def wait(j, slot):
        pltpu.make_async_copy(own.at[0], image.at[slot], image_sem.at[slot]).wait()

    out[...] = jnp.zeros_like(out)
    for j in range(DEPTH):

        @pl.when(j < total)
        def _(j=j):
            start(j, j)

    fetch_slices(a_list, a_ends, slices_a, pl.ds(0, ROWS_A))
    fetch_slices(b_list, b_ends, slices_b, pl.ds(ROWS_A, ROWS_B))
    half = lax.broadcasted_iota(jnp.int32, (8, 128), 0) // 2
    first = half == 0
    low, high, zero, down = half, half + 4, half * 0, 4 - half
    wrap = jnp.where(first, 0, 8 - half)

    def rows_of(v, index):
        return jnp.take_along_axis(v, index, axis=0, mode="promise_in_bounds")

    def waves(j):
        depth = depth_at[j]
        result = []
        for g in range(SIDE // 16 + 1):
            turns = depth * rate[8 * g : 8 * g + 8, :] + shift[8 * g : 8 * g + 8, :]
            turns = turns - jnp.round(turns)
            sq = turns * turns
            y = sq * SINE[-1] + SINE[-2]
            for term in SINE[-3::-1]:
                y = y * sq + term
            result.append(y * turns)
        return result

    def spread(s, v):
        if v < 16:
            return rows_of(s[v // 2], high if v % 2 else low)
        h = v - 16
        if h % 2:
            return rows_of(s[(15 - h) // 2], down)
        m = 8 - h // 2
        return jnp.where(first, rows_of(s[m], zero), rows_of(s[m - 1], wrap))

    def power(j, slot, k, m):
        s = waves(j)
        for g in range(ROWS // 16):
            r = pl.ds(16 * g, 16)
            wave = jnp.concatenate([spread(s, 2 * g), spread(s, 2 * g + 1)], 0)
            e = image[slot, r, :].astype(jnp.float32) + wave * fetched[j, r, :].astype(jnp.float32)
            square[m % 2, r, :] = e * e
            if g % 2:
                b = g // 2
                p = square[m % 2, pl.ds(32 * b, 16, stride=2), :] + square[m % 2, pl.ds(32 * b + 1, 16, stride=2), :]
                high_part = p.astype(jnp.bfloat16)
                q = pl.ds(SIDE * m + 16 * b, 16)
                terms[k, q, 0:128] = high_part
                terms[k, q, 128:256] = (p - high_part.astype(jnp.float32)).astype(jnp.bfloat16)

    def collect(sums, j, m):
        parts = [jnp.zeros((8, 128), jnp.float32) for _ in range(2)]
        for g in range(SIDE // 8):
            row = sums[SIDE * m + 8 * g : SIDE * m + 8 * g + 8]
            index = reach[8 * g : 8 * g + 8, :]
            parts[g % 2] = parts[g % 2] + jnp.take_along_axis(row, index, axis=1, mode="promise_in_bounds")
        out[pl.ds(j, 1), :] = jnp.sum(parts[0] + parts[1], axis=0, keepdims=True)

    def region(j, slot, k, before):
        sums = jnp.dot(terms[1 - k], within[...], preferred_element_type=jnp.float32)
        for m in range(PACK):
            power(j + m, slot + m, k, m)
            collect(sums, before + m, m)

    def step(i, carry):
        j = STEP * i
        slot = lax.rem(j, DEPTH)
        block = fetched.at[pl.ds(j, STEP)]
        pltpu.make_async_copy(own.at[pl.ds(0, STEP)], block, slice_sem.at[i]).wait()
        for m in range(STEP):
            wait(j + m, slot + m)
        region(j, slot, 0, jnp.maximum(j - PACK, 0))
        region(j + PACK, slot + PACK, 1, j)
        for m in range(STEP):

            @pl.when(j + m + DEPTH < total)
            def _(m=m):
                start(j + m + DEPTH, slot + m)

        return carry

    terms[...] = jnp.zeros_like(terms)
    lax.fori_loop(0, steps, step, 0)

    @pl.when(total > 0)
    def _():
        sums = jnp.dot(terms[1], within[...], preferred_element_type=jnp.float32)
        for m in range(PACK):
            collect(sums, total - PACK + m, m)

    disks = out[...]
    out[...] = disks - pltpu.roll(disks, 1, 1)


def shell_sums(count, image_at, a_list, b_list, a_ends, b_ends, depth, own, other, slices_a, slices_b):
    rate, shift, within, reach = tables()
    smem = pl.BlockSpec(memory_space=pltpu.SMEM)
    hbm = pl.BlockSpec(memory_space=pltpu.HBM)
    vmem = pl.BlockSpec(memory_space=pltpu.VMEM)
    return pl.pallas_call(
        shell_kernel,
        out_shape=jax.ShapeDtypeStruct((CANDIDATES, 128), jnp.float32),
        in_specs=[smem] * 7 + [hbm] * (2 + 2 * PIECES) + [vmem] * 4,
        out_specs=vmem,
        scratch_shapes=[
            pltpu.VMEM((DEPTH, ROWS, 128), jnp.bfloat16),
            pltpu.VMEM((CANDIDATES, ROWS, 128), jnp.bfloat16),
            pltpu.VMEM((2, ROWS, 128), jnp.float32),
            pltpu.VMEM((2, SIDE * PACK, 256), jnp.bfloat16),
            pltpu.SemaphoreType.DMA((DEPTH,)),
            pltpu.SemaphoreType.DMA((CANDIDATES // STEP,)),
        ],
        name="shell_sums",
    )(
        count, image_at, a_list, b_list, a_ends, b_ends, depth, own, other, *slices_a, *slices_b,
        jnp.asarray(rate), jnp.asarray(shift), jnp.asarray(within, jnp.bfloat16), jnp.asarray(reach),
    )


def ring_pairs(rings, step):
    pairs = []
    for source in range(DEVICES):
        at = {"z": source // 32, "y": source // 8 % 4, "x": source // 2 % 4, "c": source % 2}
        to = dict(at)
        ring = rings[at["c"]]
        to[ring] = (at[ring] + step) % RING
        pairs.append((source, ((to["z"] * 4 + to["y"]) * 4 + to["x"]) * 2 + to["c"]))
    return pairs


def gather_ring(x, rings):
    half = x.shape[0] // 2
    up, down = ring_pairs(rings, 1), ring_pairs(rings, -1)
    left = lax.ppermute(x, AXES, up)
    right = lax.ppermute(x, AXES, down)
    return x, right, lax.ppermute(left[:half], AXES, up), lax.ppermute(right[half:], AXES, down), left


def gather_slices(parts, orders, early):
    for phase in range(3):
        if phase:
            parts = tuple(jnp.concatenate(p, 0) for p in parts)
            parts, early = lax.optimization_barrier((parts, early))
        parts = [gather_ring(x, (o[0][phase], o[1][phase])) for x, o in zip(parts, orders)]
    return (*parts, early)


def place_of(owner, rotation, rings, core):
    here = {a: lax.axis_index(a) for a in AXES}
    ahead = {
        "z": (owner // 32 - here["z"]) % RING,
        "y": (owner // 8 % 4 - here["y"]) % RING,
        "x": (owner // 2 % 4 - here["x"]) % RING,
    }
    places = [((ahead[r[2]] * 4 + ahead[r[1]]) * 4 + ahead[r[0]]) * ROT + rotation for r in rings]
    return jnp.where(core == 0, places[0], places[1])


def by_piece(place, here, wanted, index):
    starts = np.array([0, SPAN, 2 * SPAN, 2 * SPAN + SPAN // 2, 3 * SPAN, 4 * SPAN])
    place = jnp.where(here, place, 0)
    piece = sum((place >= int(edge)).astype(jnp.int32) for edge in starts[1:PIECES])
    at = place - sum(jnp.where(piece == b, int(starts[b]), 0) for b in range(PIECES))
    piece = jnp.where(wanted, piece, PIECES)
    key = piece * CANDIDATES + index
    rank = jnp.sum((key[None, :] < key[:, None]).astype(jnp.int32), axis=1)
    entry = index * SPAN + at
    places = jnp.sum(jnp.where(rank[None, :] == index[:, None], entry[None, :], 0), axis=1)
    edges = jnp.arange(8, dtype=jnp.int32)
    return places, jnp.sum((piece[None, :] < edges[:, None]).astype(jnp.int32), axis=1)


def by_rows(x):
    lead = x.shape[:-2]
    x = x.reshape(*lead, 2, SIDE, SIDE)
    return jnp.swapaxes(x, -3, -2).reshape(*lead, ROWS, SIDE)


def body(images, slices, classes, rotations, defocus, groups):
    core = lax.axis_index("c")
    swap = [(0, 1), (1, 0)]
    facts = jnp.stack([classes, rotations, defocus, groups])
    facts = jnp.concatenate([facts, lax.ppermute(facts, "c", swap)], 1)
    own = by_rows(images)
    other = lax.ppermute(own, "c", swap)
    own_slices = by_rows(slices[0])
    slices_a, slices_b, facts = gather_slices(
        (own_slices[:, :ROWS_A], own_slices[:, ROWS_A:]), (RINGS_A, RINGS_B), facts
    )
    owner, rotation, depth, group = facts
    mine = owner % 2 == core
    index = jnp.arange(CANDIDATES, dtype=jnp.int32)
    rank = jnp.sum((mine[None, :] & (index[None, :] < index[:, None])).astype(jnp.int32), axis=1)
    count = jnp.sum(mine.astype(jnp.int32)).reshape(1)
    chosen = (rank[None, :] == index[:, None]) & mine[None, :]
    a_place = place_of(owner, rotation, RINGS_A, core)
    b_place = place_of(owner, rotation, RINGS_B, core)

    def packed(values):
        return jnp.sum(jnp.where(chosen, values[None, :], 0), axis=1)

    depth = packed(depth).astype(jnp.float32)
    here = index < count
    group = jnp.where(here, packed(group), -1)
    whole = (count + STEP - 1) // STEP * STEP
    a_list, a_ends = by_piece(packed(a_place), here, index < whole, index)
    b_list, b_ends = by_piece(packed(b_place), here, index < whole, index)
    sums = shell_sums(
        whole, packed(index), a_list, b_list, a_ends, b_ends, depth, own, other, slices_a, slices_b
    )
    lane = jnp.arange(128, dtype=jnp.int32)
    sums = jnp.where(lane < SHELLS, sums, jnp.where(lane == SHELLS, 1.0, 0.0))
    member = (jnp.arange(GROUPS, dtype=jnp.int32)[:, None] == group[None, :]).astype(jnp.float32)
    partial = jnp.dot(member, sums, precision=lax.Precision.HIGHEST, preferred_element_type=jnp.float32)
    arrived = lax.all_to_all(partial.reshape(DEVICES, GROUPS_DEV, 128), AXES, 0, 0, tiled=True)
    own_groups = jnp.sum(arrived, axis=0)
    return own_groups[:, :SHELLS] / (2.0 * own_groups[:, SHELLS : SHELLS + 1] * jnp.asarray(shell_pixels()))


def solution(mesh):
    finer = Mesh(mesh.devices.reshape(4, 4, 4, 2), AXES)
    placed = (
        P(AXES, None, None),
        P(AXES, None, None, None),
        P(AXES),
        P(AXES),
        P(AXES),
        P(AXES),
    )
    return jax.shard_map(body, mesh=finer, in_specs=placed, out_specs=P(AXES, None), check_vma=False)
```

```python
import functools
import math

import jax
import jax.numpy as jnp
import numpy as np
from jax import lax
from jax.experimental import pallas as pl
from jax.experimental.pallas import tpu as pltpu
from jax.sharding import Mesh
from jax.sharding import PartitionSpec as P


AXES = ("z", "y", "x", "c")
RING = 4
SIDE = 128
HALF = SIDE // 2
SHELLS = 64
ROT = 4
P_DEV = 128
GROUPS_DEV = 8
DEVICES = 128
GROUPS = GROUPS_DEV * DEVICES
CANDIDATES = 2 * P_DEV

PIXEL_SIZE = 1.5
WAVELENGTH = 0.0197
SPHERICAL = 27000000.0
AMPLITUDE = 0.1

ROWS = 2 * SIDE
ROWS_A = 176
ROWS_B = ROWS - ROWS_A
RINGS_A = (("y", "z", "x"), ("x", "y", "z"))
RINGS_B = (("x", "z", "y"), ("z", "x", "y"))

DEPTH = 32
PACK = 4
STEP = 2 * PACK
RESULTS = CANDIDATES + STEP
A_ENDS, B_ENDS, IMAGE_AT = 16, 32, 48
A_LIST, B_LIST, DEPTH_AT = IMAGE_AT + RESULTS, IMAGE_AT + 2 * RESULTS, IMAGE_AT + 3 * RESULTS
LENGTHS = (16, 16, 16, 8, 8) + 3 * (16, 32, 16)
ALL = tuple(range(len(LENGTHS)))
EARLY = tuple(b for b in ALL if b not in (8, 9, 10))
SPAN = 64
NOWHERE = 127


def sine_terms():
    turns = np.cos(np.linspace(0, np.pi, 4001)) * 0.5
    turns = turns[np.abs(turns) > 1e-9]
    basis = np.stack([np.abs(turns) * turns ** (2 * k) for k in range(6)], 1)
    target = np.sin(2 * np.pi * turns) / turns * np.abs(turns)
    return [float(c) for c in np.linalg.lstsq(basis, target, rcond=None)[0]]


SINE = sine_terms()


def frequencies():
    offsets = np.arange(SIDE)
    return np.where(offsets < SIDE // 2, offsets, offsets - SIDE)


def tables():
    freq = frequencies()
    radius_sq = (freq[:, None] ** 2 + freq[None, :] ** 2).astype(np.float64)
    spatial = radius_sq / (SIDE * PIXEL_SIZE) ** 2
    rate = 0.5 * WAVELENGTH * spatial
    shift = -0.25 * SPHERICAL * WAVELENGTH**3 * spatial**2 + math.asin(AMPLITUDE) / (2 * math.pi)
    within = np.zeros((SIDE, 128), np.float32)
    for w in range(SIDE // 2 + 1):
        within[:, w] = np.abs(freq) <= w
    reach = np.full((HALF + 8, 128), NOWHERE, np.int32)
    for a in range(HALF + 1):
        for s in range(SHELLS):
            left = (s + 1) ** 2 - 1 - int(freq[a]) ** 2
            if left >= 0:
                reach[a, s] = min(math.isqrt(left), SIDE // 2)
    half = HALF + 8
    return (
        rate[:half].astype(np.float32),
        shift[:half].astype(np.float32),
        np.concatenate([within, within], 0),
        reach,
    )


def shell_pixels():
    freq = frequencies()
    radius_sq = freq[:, None] ** 2 + freq[None, :] ** 2
    return np.array(
        [((s * s <= radius_sq) & (radius_sq < (s + 1) ** 2)).sum() for s in range(SHELLS)], np.float32
    )


def shell_kernel(
    plan_ref, *refs, held, first,
):
    done, refs = (None, refs) if first else (refs[0], refs[1:])
    own, other, *refs = refs
    pieces = len(held[0]) + len(held[1])
    slices_a, slices_b = refs[: len(held[0])], refs[len(held[0]) : pieces]
    constants, (out, *scratch) = refs[pieces : pieces + 4], refs[pieces + 4 :]
    tables_here, (image, fetched, square, terms, image_sem, slice_sem, table_sem) = scratch[:4], scratch[4:]
    rate, shift, within, reach = tables_here
    begin, total = plan_ref[0], plan_ref[1]

    def table_copies():
        return [
            pltpu.make_async_copy(there, here, table_sem.at[i])
            for i, (there, here) in enumerate(zip(constants, tables_here))
        ]

    def fetch_slices(places, ends, numbers, parts, rows):
        for b, part in zip(numbers, parts):
            low, high = plan_ref[ends + b], plan_ref[ends + b + 1]

            def fetch(t, part=part):
                entry = plan_ref[places + t]
                j, at = entry // SPAN, entry % SPAN
                pltpu.make_async_copy(part.at[at], fetched.at[j, rows], slice_sem.at[j // STEP]).start()

            def fetch_some(i, carry, fetch=fetch, low=low):
                for k in range(4):
                    fetch(low + 4 * i + k)
                return carry

            def fetch_one(t, carry, fetch=fetch):
                fetch(t)
                return carry

            fours = (high - low) // 4
            lax.fori_loop(0, fours, fetch_some, 0)
            lax.fori_loop(low + 4 * fours, high, fetch_one, 0)

    def start(j, slot):
        at = plan_ref[IMAGE_AT + j]

        @pl.when(at < P_DEV)
        def _():
            pltpu.make_async_copy(own.at[at], image.at[slot], image_sem.at[slot]).start()

        @pl.when(at >= P_DEV)
        def _():
            pltpu.make_async_copy(other.at[at - P_DEV], image.at[slot], image_sem.at[slot]).start()

    def wait(slot):
        pltpu.make_async_copy(own.at[0], image.at[slot], image_sem.at[slot]).wait()

    for copy in table_copies():
        copy.start()

    def start_early(j, carry):
        start(j, lax.rem(j, DEPTH))
        return carry

    lax.fori_loop(begin, jnp.minimum(begin + DEPTH, total), start_early, 0)
    fetch_slices(A_LIST, A_ENDS, held[0], slices_a, pl.ds(0, ROWS_A))
    fetch_slices(B_LIST, B_ENDS, held[1], slices_b, pl.ds(ROWS_A, ROWS_B))
    sublane = lax.broadcasted_iota(jnp.int32, (8, 128), 0)
    out[...] = jnp.zeros_like(out) if first else done[...]
    half, top = sublane // 2, sublane == 0
    back = jnp.where(top, 0, 8 - sublane)
    first = half == 0
    low, high, zero, down = half, half + 4, half * 0, 4 - half
    wrap = jnp.where(first, 0, 8 - half)

    def rows_of(v, index):
        return jnp.take_along_axis(v, index, axis=0, mode="promise_in_bounds")

    def waves(j):
        depth = plan_ref[DEPTH_AT + j].astype(jnp.float32)
        result = []
        for g in range(SIDE // 16 + 1):
            turns = depth * rate[8 * g : 8 * g + 8, :] + shift[8 * g : 8 * g + 8, :]
            turns = turns - jnp.round(turns)
            sq = turns * turns
            y = sq * SINE[-1] + SINE[-2]
            for term in SINE[-3::-1]:
                y = y * sq + term
            result.append(y * turns)
        return result

    def spread(s, v):
        if v < 16:
            return rows_of(s[v // 2], high if v % 2 else low)
        h = v - 16
        if h % 2:
            return rows_of(s[(15 - h) // 2], down)
        m = 8 - h // 2
        return jnp.where(first, rows_of(s[m], zero), rows_of(s[m - 1], wrap))

    def keep(k, at, pair):
        p = jnp.concatenate(pair, 0)
        high_part = p.astype(jnp.bfloat16)
        terms[k, at : at + 16, 0:128] = high_part
        terms[k, at : at + 16, 128:256] = (p - high_part.astype(jnp.float32)).astype(jnp.bfloat16)

    def power(j, slot, k, m):
        s = waves(j)

        def pixel_power(g):
            for h in range(2):
                v = 4 * g + 2 * h
                r = pl.ds(8 * v, 16)
                wave = jnp.concatenate([spread(s, v), spread(s, v + 1)], 0)
                e = image[slot, r, :].astype(jnp.float32) + wave * fetched[j, r, :].astype(jnp.float32)
                square[m % 2, r, :] = e * e
            both = [square[m % 2, pl.ds(32 * g + part, 16, stride=2), :] for part in range(2)]
            p = both[0] + both[1]
            return [p[:8], p[8:]]

        turned = [rows_of(p, back) for g in range(4, 8) for p in pixel_power(g)]
        turned.append(jnp.zeros((8, 128), jnp.float32))
        for g in range(4):
            near = pixel_power(g)
            for h in range(2):
                v = 2 * g + h
                near[h] = near[h] + jnp.where(top, turned[8 - v], turned[7 - v])
            keep(k, HALF * m + 16 * g, near)
        return jnp.where(top, turned[0], 0.0)

    def keep_edges(edges, k):
        for at in range(0, PACK, 2):
            keep(k, HALF * PACK + 8 * at, edges[at : at + 2])

    def collect(sums, j, m):
        parts = [jnp.zeros((8, 128), jnp.float32) for _ in range(2)]
        starts = [HALF * m + 8 * g for g in range(8)] + [HALF * PACK + 8 * m]
        for g, at in enumerate(starts):
            index = reach[8 * g : 8 * g + 8, :]
            found = jnp.take_along_axis(sums[at : at + 8], index, axis=1, mode="promise_in_bounds")
            parts[g % 2] = parts[g % 2] + found
        out[pl.ds(j, 1), :] = jnp.sum(parts[0] + parts[1], axis=0, keepdims=True)

    def region(j, slot, k, before):
        sums = jnp.dot(terms[1 - k], within[...], preferred_element_type=jnp.float32)
        edges = []
        for m in range(PACK):
            edges.append(power(j + m, slot + m, k, m))
            collect(sums, before + m, m)
        keep_edges(edges, k)

    def step(i, carry):
        j = STEP * i
        slot = lax.rem(j, DEPTH)
        block = fetched.at[pl.ds(j, STEP)]
        pltpu.make_async_copy(own.at[pl.ds(0, STEP)], block, slice_sem.at[i]).wait()
        for m in range(STEP):
            wait(slot + m)
        region(j, slot, 0, jnp.maximum(j - PACK, begin))
        region(j + PACK, slot + PACK, 1, j)
        for m in range(STEP):

            @pl.when(j + m + DEPTH < total)
            def _(m=m):
                start(j + m + DEPTH, slot + m)

        return carry

    terms[...] = jnp.zeros_like(terms)
    for copy in table_copies():
        copy.wait()
    lax.fori_loop(begin // STEP, total // STEP, step, 0)

    @pl.when(total > begin)
    def _():
        sums = jnp.dot(terms[1], within[...], preferred_element_type=jnp.float32)
        for m in range(PACK):
            collect(sums, total - PACK + m, m)


def shell_sums(held, plan, done, own, other, slices_a, slices_b):
    before = () if done is None else (done,)
    rate, shift, within, reach = tables()
    constants = jnp.asarray(rate), jnp.asarray(shift), jnp.asarray(within, jnp.bfloat16), jnp.asarray(reach)
    smem = pl.BlockSpec(memory_space=pltpu.SMEM)
    hbm = pl.BlockSpec(memory_space=pltpu.HBM)
    vmem = pl.BlockSpec(memory_space=pltpu.VMEM)
    return pl.pallas_call(
        functools.partial(shell_kernel, held=held, first=done is None),
        out_shape=jax.ShapeDtypeStruct((RESULTS, 128), jnp.float32),
        in_specs=[smem] + [vmem] * len(before) + [hbm] * (2 + len(held[0]) + len(held[1]) + len(constants)),
        out_specs=vmem,
        scratch_shapes=[
            *(pltpu.VMEM(c.shape, c.dtype) for c in constants),
            pltpu.VMEM((DEPTH, ROWS, 128), jnp.bfloat16),
            pltpu.VMEM((RESULTS, ROWS, 128), jnp.bfloat16),
            pltpu.VMEM((2, ROWS, 128), jnp.float32),
            pltpu.VMEM((2, (HALF + 8) * PACK, 256), jnp.bfloat16),
            pltpu.SemaphoreType.DMA((DEPTH,)),
            pltpu.SemaphoreType.DMA((RESULTS // STEP,)),
            pltpu.SemaphoreType.DMA((len(constants),)),
        ],
    )(
        plan, *before, own, other,
        *(slices_a[b] for b in held[0]), *(slices_b[b] for b in held[1]), *constants,
    )


def ring_pairs(rings, step):
    pairs = []
    for source in range(DEVICES):
        at = {"z": source // 32, "y": source // 8 % 4, "x": source // 2 % 4, "c": source % 2}
        to = dict(at)
        ring = rings[at["c"]]
        to[ring] = (at[ring] + step) % RING
        pairs.append((source, ((to["z"] * 4 + to["y"]) * 4 + to["x"]) * 2 + to["c"]))
    return pairs


def send(x, rings, step):
    return lax.ppermute(x, AXES, ring_pairs(rings, step))


def joined(parts):
    return jnp.concatenate(parts, 0)


def last_ring(own, near, rest, rings):
    parts = own, near, rest
    left = [send(x, rings, 1) for x in parts]
    right = [send(x, rings, -1) for x in parts]
    far = (send(right[0], rings, -1), send(left[1], rings, 1), send(right[2], rings, -1))
    return (*right, *far, *left)


def gather_part(x, rings):
    first, second, third = zip(*rings)
    x = x, send(x, first, -1), send(x, first, 2), send(x, first, 1)
    block = joined(x)
    half = block.shape[0] // 2
    right, left = send(block, second, -1), send(block, second, 1)
    far = send(left[:half], second, 1), send(right[half:], second, -1)
    near, rest = joined((right, left)), joined(far)
    return (block, right, left, *far, *last_ring(block, near, rest, third))


def place_of(owner, rotation, rings, core):
    here = {a: lax.axis_index(a) for a in AXES}
    ahead = {
        "z": (owner // 32 - here["z"]) % RING,
        "y": (owner // 8 % 4 - here["y"]) % RING,
        "x": (owner // 2 % 4 - here["x"]) % RING,
    }
    places = [
        ((ahead[r[2]] * 4 + (ahead[r[1]] ^ (ahead[r[1]] >> 1))) * 4 + ahead[r[0]]) * ROT + rotation for r in rings
    ]
    return jnp.where(core == 0, places[0], places[1])


def by_piece(place, here, wanted, index):
    starts = np.cumsum((0,) + LENGTHS)
    place = jnp.where(here, place, 0)
    piece = sum((place >= int(edge)).astype(jnp.int32) for edge in starts[1:-1])
    at = place - sum(jnp.where(piece == b, int(starts[b]), 0) for b in range(len(LENGTHS)))
    piece = jnp.where(wanted, piece, len(LENGTHS))
    key = piece * RESULTS + index
    rank = jnp.sum((key[None, :] < key[:, None]).astype(jnp.int32), axis=1)
    entry = index * SPAN + at
    places = jnp.sum(jnp.where(rank[None, :] == index[:, None], entry[None, :], 0), axis=1)
    edges = jnp.arange(16, dtype=jnp.int32)
    return places, jnp.sum((piece[None, :] < edges[:, None]).astype(jnp.int32), axis=1)


def swapped(x):
    return lax.ppermute(x, "c", [(0, 1), (1, 0)])


def by_rows(x):
    lead = x.shape[:-2]
    x = x.reshape(*lead, 2, SIDE, SIDE)
    return jnp.swapaxes(x, -3, -2).reshape(*lead, ROWS, SIDE)


def plan(facts, core):
    owner, rotation, depth, group = facts
    mine = owner % 2 == core
    a_place = place_of(owner, rotation, RINGS_A, core)
    b_place = place_of(owner, rotation, RINGS_B, core)
    late = mine & ((a_place // SPAN == 2) | (b_place // SPAN == 2))
    early = mine & ~late

    def ranks(mask):
        i = jnp.arange(CANDIDATES, dtype=jnp.int32)
        before = (i[None, :] < i[:, None]) & mask[None, :]
        return jnp.sum(before.astype(jnp.int32), axis=1), jnp.sum(mask.astype(jnp.int32))

    def whole_steps(n):
        return (n + STEP - 1) // STEP * STEP

    early_rank, early_count = ranks(early)
    late_rank, late_count = ranks(late)
    middle = whole_steps(early_count)
    end = middle + whole_steps(late_count)
    index = jnp.arange(RESULTS, dtype=jnp.int32)
    row = jnp.where(early, early_rank, jnp.where(late, middle + late_rank, -1))
    chosen = row[None, :] == index[:, None]

    def packed(values):
        return jnp.sum(jnp.where(chosen, values[None, :], 0), axis=1)

    depth = packed(depth)
    here = (index < early_count) | ((index >= middle) & (index < middle + late_count))
    group = jnp.where(here, packed(group), -1)
    image_at = packed(jnp.arange(CANDIDATES, dtype=jnp.int32))
    a_place, b_place = packed(a_place), packed(b_place)
    plans = []
    for begin, until in ((jnp.int32(0), middle), (middle, end)):
        wanted = (index >= begin) & (index < until)
        a_list, a_ends = by_piece(a_place, here, wanted, index)
        b_list, b_ends = by_piece(b_place, here, wanted, index)
        head = jnp.arange(16, dtype=jnp.int32)
        span = jnp.where(head == 0, begin, until)
        plans.append(jnp.concatenate([span, a_ends, b_ends, image_at, a_list, b_list, depth]))
    return group, plans


def body(images, slices, classes, rotations, defocus, groups):
    core = lax.axis_index("c")
    facts = jnp.stack([classes, rotations, defocus, groups])
    facts = jnp.concatenate([facts, swapped(facts)], 1)
    own = by_rows(images)
    other = swapped(own)
    own_slices = by_rows(slices[0])
    slices_a = gather_part(own_slices[:, :ROWS_A], RINGS_A)
    slices_b = gather_part(own_slices[:, ROWS_A:], RINGS_B)
    group, plans = plan(facts, core)
    sums = None
    for held, one in (((EARLY, EARLY), plans[0]), ((ALL, ALL), plans[1])):
        sums = shell_sums(held, one, sums, own, other, slices_a, slices_b)
    lane = jnp.arange(128, dtype=jnp.int32)
    inner = jnp.pad(sums[:, : SHELLS - 1], ((0, 0), (1, 128 - SHELLS)))
    sums = jnp.where(lane < SHELLS, sums - inner, jnp.where(lane == SHELLS, 1.0, 0.0))
    high = lax.reduce_precision(sums, 8, 7)
    parts = jnp.concatenate([high, sums - high], 1).astype(jnp.bfloat16)
    member = (jnp.arange(GROUPS, dtype=jnp.int32)[:, None] == group[None, :]).astype(jnp.bfloat16)
    partial = jnp.dot(member, parts, preferred_element_type=jnp.float32)
    partial = partial[:, :128] + partial[:, 128:]
    arrived = lax.all_to_all(partial.reshape(DEVICES, GROUPS_DEV, 128), AXES, 0, 0, tiled=True)
    own_groups = jnp.sum(arrived, axis=0)
    return own_groups[:, :SHELLS] / (2.0 * own_groups[:, SHELLS : SHELLS + 1] * jnp.asarray(shell_pixels()))


def solution(mesh):
    finer = Mesh(mesh.devices.reshape(4, 4, 4, 2), AXES)
    placed = (
        P(AXES, None, None),
        P(AXES, None, None, None),
        P(AXES),
        P(AXES),
        P(AXES),
        P(AXES),
    )
    return jax.shard_map(body, mesh=finer, in_specs=placed, out_specs=P(AXES, None), check_vma=False)
```

```python
import functools
import math

import jax
import jax.numpy as jnp
import numpy as np
from jax import lax
from jax.experimental import pallas as pl
from jax.experimental.pallas import tpu as pltpu
from jax.sharding import Mesh
from jax.sharding import PartitionSpec as P


AXES = ("z", "y", "x", "c")
RING = 4
SIDE = 128
HALF = SIDE // 2
SHELLS = 64
ROT = 4
P_DEV = 128
GROUPS_DEV = 8
DEVICES = 128
GROUPS = GROUPS_DEV * DEVICES
CANDIDATES = 2 * P_DEV

PIXEL_SIZE = 1.5
WAVELENGTH = 0.0197
SPHERICAL = 27000000.0
AMPLITUDE = 0.1

ROWS = 2 * SIDE
ROWS_A = 176
ROWS_B = ROWS - ROWS_A
RINGS_A = (("y", "z", "x"), ("x", "y", "z"))
RINGS_B = (("x", "z", "y"), ("z", "x", "y"))

DEPTH = 32
PACK = 4
STEP = 2 * PACK
RESULTS = CANDIDATES + STEP
A_ENDS, B_ENDS, IMAGE_AT = 16, 32, 48
A_LIST, B_LIST, DEPTH_AT = IMAGE_AT + RESULTS, IMAGE_AT + 2 * RESULTS, IMAGE_AT + 3 * RESULTS
LENGTHS = (16, 16, 16, 8, 8) + 3 * (16, 32, 16)
ALL = tuple(range(len(LENGTHS)))
EARLY = tuple(b for b in ALL if b not in (8, 9, 10))
SPAN = 64
NOWHERE = 127
COLUMNS = 80


def sine_terms():
    turns = np.cos(np.linspace(0, np.pi, 4001)) * 0.5
    turns = turns[np.abs(turns) > 1e-9]
    basis = np.stack([np.abs(turns) * turns ** (2 * k) for k in range(6)], 1)
    target = np.sin(2 * np.pi * turns) / turns * np.abs(turns)
    return [float(c) for c in np.linalg.lstsq(basis, target, rcond=None)[0]]


SINE = sine_terms()


def frequencies():
    offsets = np.arange(SIDE)
    return np.where(offsets < SIDE // 2, offsets, offsets - SIDE)


def tables():
    freq = frequencies()
    radius_sq = (freq[:, None] ** 2 + freq[None, :] ** 2).astype(np.float64)
    spatial = radius_sq / (SIDE * PIXEL_SIZE) ** 2
    rate = 0.5 * WAVELENGTH * spatial
    shift = -0.25 * SPHERICAL * WAVELENGTH**3 * spatial**2 + math.asin(AMPLITUDE) / (2 * math.pi)
    within = np.zeros((SIDE, 128), np.float32)
    for w in range(SIDE // 2 + 1):
        within[:, w] = np.abs(freq) <= w
    reach = np.full((HALF + 8, 128), NOWHERE, np.int32)
    for a in range(HALF + 1):
        for s in range(SHELLS):
            left = (s + 1) ** 2 - 1 - int(freq[a]) ** 2
            if left >= 0:
                reach[a, s] = min(math.isqrt(left), SIDE // 2)
    half = HALF + 8
    return (
        rate[:half].astype(np.float32),
        shift[:half].astype(np.float32),
        np.concatenate([within, within], 0),
        reach,
    )


def shell_pixels():
    freq = frequencies()
    radius_sq = freq[:, None] ** 2 + freq[None, :] ** 2
    return np.array(
        [((s * s <= radius_sq) & (radius_sq < (s + 1) ** 2)).sum() for s in range(SHELLS)], np.float32
    )


def shell_kernel(
    plan_ref, *refs, held, first,
):
    done, refs = (None, refs) if first else (refs[0], refs[1:])
    own, other, *refs = refs
    pieces = len(held[0]) + len(held[1])
    slices_a, slices_b = refs[: len(held[0])], refs[len(held[0]) : pieces]
    constants, (out, *scratch) = refs[pieces : pieces + 4], refs[pieces + 4 :]
    tables_here, (image, fetched, square, terms, image_sem, slice_sem, table_sem) = scratch[:4], scratch[4:]
    rate, shift, within, reach = tables_here
    begin, total = plan_ref[0], plan_ref[1]

    def table_copies():
        return [
            pltpu.make_async_copy(there, here, table_sem.at[i])
            for i, (there, here) in enumerate(zip(constants, tables_here))
        ]

    def fetch_slices(places, ends, numbers, parts, rows):
        for b, part in zip(numbers, parts):
            low, high = plan_ref[ends + b], plan_ref[ends + b + 1]

            def fetch(t, part=part):
                entry = plan_ref[places + t]
                j, at = entry // SPAN, entry % SPAN
                pltpu.make_async_copy(part.at[at], fetched.at[j, rows], slice_sem.at[j // STEP]).start()

            def fetch_some(i, carry, fetch=fetch, low=low):
                for k in range(4):
                    fetch(low + 4 * i + k)
                return carry

            def fetch_one(t, carry, fetch=fetch):
                fetch(t)
                return carry

            fours = (high - low) // 4
            lax.fori_loop(0, fours, fetch_some, 0)
            lax.fori_loop(low + 4 * fours, high, fetch_one, 0)

    def start(j, slot):
        at = plan_ref[IMAGE_AT + j]

        @pl.when(at < P_DEV)
        def _():
            pltpu.make_async_copy(own.at[at], image.at[slot], image_sem.at[slot]).start()

        @pl.when(at >= P_DEV)
        def _():
            pltpu.make_async_copy(other.at[at - P_DEV], image.at[slot], image_sem.at[slot]).start()

    def wait(slot):
        pltpu.make_async_copy(own.at[0], image.at[slot], image_sem.at[slot]).wait()

    for copy in table_copies():
        copy.start()

    def start_early(j, carry):
        start(j, lax.rem(j, DEPTH))
        return carry

    lax.fori_loop(begin, jnp.minimum(begin + DEPTH, total), start_early, 0)
    fetch_slices(A_LIST, A_ENDS, held[0], slices_a, pl.ds(0, ROWS_A))
    fetch_slices(B_LIST, B_ENDS, held[1], slices_b, pl.ds(ROWS_A, ROWS_B))
    sublane = lax.broadcasted_iota(jnp.int32, (8, 128), 0)
    out[...] = jnp.zeros_like(out) if first else done[...]
    half, top = sublane // 2, sublane == 0
    back = jnp.where(top, 0, 8 - sublane)
    first = half == 0
    low, high, zero, down = half, half + 4, half * 0, 4 - half
    wrap = jnp.where(first, 0, 8 - half)

    def rows_of(v, index):
        return jnp.take_along_axis(v, index, axis=0, mode="promise_in_bounds")

    def waves(j):
        depth = plan_ref[DEPTH_AT + j].astype(jnp.float32)
        result = []
        for g in range(SIDE // 16 + 1):
            turns = depth * rate[8 * g : 8 * g + 8, :] + shift[8 * g : 8 * g + 8, :]
            turns = turns - jnp.round(turns)
            sq = turns * turns
            y = sq * SINE[-1] + SINE[-2]
            for term in SINE[-3::-1]:
                y = y * sq + term
            result.append(y * turns)
        return result

    def spread(s, v):
        if v < 16:
            return rows_of(s[v // 2], high if v % 2 else low)
        h = v - 16
        if h % 2:
            return rows_of(s[(15 - h) // 2], down)
        m = 8 - h // 2
        return jnp.where(first, rows_of(s[m], zero), rows_of(s[m - 1], wrap))

    def keep(k, at, pair):
        p = jnp.concatenate(pair, 0)
        high_part = p.astype(jnp.bfloat16)
        terms[k, at : at + 16, 0:128] = high_part
        terms[k, at : at + 16, 128:256] = (p - high_part.astype(jnp.float32)).astype(jnp.bfloat16)

    def power(j, slot, k, m):
        s = waves(j)

        def pixel_power(g):
            for h in range(2):
                v = 4 * g + 2 * h
                r = pl.ds(8 * v, 16)
                wave = jnp.concatenate([spread(s, v), spread(s, v + 1)], 0)
                e = image[slot, r, :].astype(jnp.float32) + wave * fetched[j, r, :].astype(jnp.float32)
                square[m % 2, r, :] = e * e
            both = [square[m % 2, pl.ds(32 * g + part, 16, stride=2), :] for part in range(2)]
            p = both[0] + both[1]
            return [p[:8], p[8:]]

        turned = [rows_of(p, back) for g in range(4, 8) for p in pixel_power(g)]
        turned.append(jnp.zeros((8, 128), jnp.float32))
        for g in range(4):
            near = pixel_power(g)
            for h in range(2):
                v = 2 * g + h
                near[h] = near[h] + jnp.where(top, turned[8 - v], turned[7 - v])
            keep(k, HALF * m + 16 * g, near)
        return jnp.where(top, turned[0], 0.0)

    def keep_edges(edges, k):
        for at in range(0, PACK, 2):
            keep(k, HALF * PACK + 8 * at, edges[at : at + 2])

    def collect(sums, j, m):
        parts = [jnp.zeros((8, 128), jnp.float32) for _ in range(2)]
        starts = [HALF * m + 8 * g for g in range(8)] + [HALF * PACK + 8 * m]
        for g, at in enumerate(starts):
            index = reach[8 * g : 8 * g + 8, :]
            found = jnp.take_along_axis(sums[at : at + 8], index, axis=1, mode="promise_in_bounds")
            parts[g % 2] = parts[g % 2] + found
        out[pl.ds(j, 1), :] = jnp.sum(parts[0] + parts[1], axis=0, keepdims=True)

    def region(j, slot, k, before):
        sums = jnp.dot(terms[1 - k], within[...], preferred_element_type=jnp.float32)
        edges = []
        for m in range(PACK):
            edges.append(power(j + m, slot + m, k, m))
            collect(sums, before + m, m)
        keep_edges(edges, k)

    def step(i, carry):
        j = STEP * i
        slot = lax.rem(j, DEPTH)
        block = fetched.at[pl.ds(j, STEP)]
        pltpu.make_async_copy(own.at[pl.ds(0, STEP)], block, slice_sem.at[i]).wait()
        for m in range(STEP):
            wait(slot + m)
        region(j, slot, 0, jnp.maximum(j - PACK, begin))
        region(j + PACK, slot + PACK, 1, j)
        for m in range(STEP):

            @pl.when(j + m + DEPTH < total)
            def _(m=m):
                start(j + m + DEPTH, slot + m)

        return carry

    terms[...] = jnp.zeros_like(terms)
    for copy in table_copies():
        copy.wait()
    lax.fori_loop(begin // STEP, total // STEP, step, 0)

    @pl.when(total > begin)
    def _():
        sums = jnp.dot(terms[1], within[...], preferred_element_type=jnp.float32)
        for m in range(PACK):
            collect(sums, total - PACK + m, m)


def shell_sums(held, plan, done, own, other, slices_a, slices_b):
    before = () if done is None else (done,)
    rate, shift, within, reach = tables()
    constants = jnp.asarray(rate), jnp.asarray(shift), jnp.asarray(within, jnp.bfloat16), jnp.asarray(reach)
    smem = pl.BlockSpec(memory_space=pltpu.SMEM)
    hbm = pl.BlockSpec(memory_space=pltpu.HBM)
    vmem = pl.BlockSpec(memory_space=pltpu.VMEM)
    return pl.pallas_call(
        functools.partial(shell_kernel, held=held, first=done is None),
        out_shape=jax.ShapeDtypeStruct((RESULTS, 128), jnp.float32),
        in_specs=[smem] + [vmem] * len(before) + [hbm] * (2 + len(held[0]) + len(held[1]) + len(constants)),
        out_specs=vmem,
        scratch_shapes=[
            *(pltpu.VMEM(c.shape, c.dtype) for c in constants),
            pltpu.VMEM((DEPTH, ROWS, 128), jnp.bfloat16),
            pltpu.VMEM((RESULTS, ROWS, 128), jnp.bfloat16),
            pltpu.VMEM((2, ROWS, 128), jnp.float32),
            pltpu.VMEM((2, (HALF + 8) * PACK, 256), jnp.bfloat16),
            pltpu.SemaphoreType.DMA((DEPTH,)),
            pltpu.SemaphoreType.DMA((RESULTS // STEP,)),
            pltpu.SemaphoreType.DMA((len(constants),)),
        ],
    )(
        plan, *before, own, other,
        *(slices_a[b] for b in held[0]), *(slices_b[b] for b in held[1]), *constants,
    )


def ring_pairs(rings, step):
    pairs = []
    for source in range(DEVICES):
        at = {"z": source // 32, "y": source // 8 % 4, "x": source // 2 % 4, "c": source % 2}
        to = dict(at)
        ring = rings[at["c"]]
        to[ring] = (at[ring] + step) % RING
        pairs.append((source, ((to["z"] * 4 + to["y"]) * 4 + to["x"]) * 2 + to["c"]))
    return pairs


def send(x, rings, step):
    return lax.ppermute(x, AXES, ring_pairs(rings, step))


def joined(parts):
    return jnp.concatenate(parts, 0)


def last_ring(own, near, rest, rings):
    parts = own, near, rest
    left = [send(x, rings, 1) for x in parts]
    right = [send(x, rings, -1) for x in parts]
    far = (send(right[0], rings, -1), send(left[1], rings, 1), send(right[2], rings, -1))
    return (*right, *far, *left)


def gather_part(x, rings):
    first, second, third = zip(*rings)
    x = x, send(x, first, -1), send(x, first, 2), send(x, first, 1)
    block = joined(x)
    half = block.shape[0] // 2
    right, left = send(block, second, -1), send(block, second, 1)
    far = send(left[:half], second, 1), send(right[half:], second, -1)
    near, rest = joined((right, left)), joined(far)
    return (block, right, left, *far, *last_ring(block, near, rest, third))


def place_of(owner, rotation, rings, core):
    here = {a: lax.axis_index(a) for a in AXES}
    ahead = {
        "z": (owner // 32 - here["z"]) % RING,
        "y": (owner // 8 % 4 - here["y"]) % RING,
        "x": (owner // 2 % 4 - here["x"]) % RING,
    }
    places = [
        ((ahead[r[2]] * 4 + (ahead[r[1]] ^ (ahead[r[1]] >> 1))) * 4 + ahead[r[0]]) * ROT + rotation for r in rings
    ]
    return jnp.where(core == 0, places[0], places[1])


def by_piece(place, here, wanted, index):
    starts = np.cumsum((0,) + LENGTHS)
    place = jnp.where(here, place, 0)
    piece = sum((place >= int(edge)).astype(jnp.int32) for edge in starts[1:-1])
    at = place - sum(jnp.where(piece == b, int(starts[b]), 0) for b in range(len(LENGTHS)))
    piece = jnp.where(wanted, piece, len(LENGTHS))
    key = piece * RESULTS + index
    rank = jnp.sum((key[None, :] < key[:, None]).astype(jnp.int32), axis=1)
    entry = index * SPAN + at
    places = jnp.sum(jnp.where(rank[None, :] == index[:, None], entry[None, :], 0), axis=1)
    edges = jnp.arange(16, dtype=jnp.int32)
    return places, jnp.sum((piece[None, :] < edges[:, None]).astype(jnp.int32), axis=1)


def swapped(x):
    return lax.ppermute(x, "c", [(0, 1), (1, 0)])


def by_rows(x):
    lead = x.shape[:-2]
    x = x.reshape(*lead, 2, SIDE, SIDE)
    return jnp.swapaxes(x, -3, -2).reshape(*lead, ROWS, SIDE)


def plan(facts, core):
    owner, rotation, depth, group = facts
    mine = owner % 2 == core
    a_place = place_of(owner, rotation, RINGS_A, core)
    b_place = place_of(owner, rotation, RINGS_B, core)
    late = mine & ((a_place // SPAN == 2) | (b_place // SPAN == 2))
    early = mine & ~late

    def ranks(mask):
        i = jnp.arange(CANDIDATES, dtype=jnp.int32)
        before = (i[None, :] < i[:, None]) & mask[None, :]
        return jnp.sum(before.astype(jnp.int32), axis=1), jnp.sum(mask.astype(jnp.int32))

    def whole_steps(n):
        return (n + STEP - 1) // STEP * STEP

    early_rank, early_count = ranks(early)
    late_rank, late_count = ranks(late)
    middle = whole_steps(early_count)
    end = middle + whole_steps(late_count)
    index = jnp.arange(RESULTS, dtype=jnp.int32)
    row = jnp.where(early, early_rank, jnp.where(late, middle + late_rank, -1))
    chosen = row[None, :] == index[:, None]

    def packed(values):
        return jnp.sum(jnp.where(chosen, values[None, :], 0), axis=1)

    depth = packed(depth)
    here = (index < early_count) | ((index >= middle) & (index < middle + late_count))
    group = jnp.where(here, packed(group), -1)
    image_at = packed(jnp.arange(CANDIDATES, dtype=jnp.int32))
    a_place, b_place = packed(a_place), packed(b_place)
    plans = []
    for begin, until in ((jnp.int32(0), middle), (middle, end)):
        wanted = (index >= begin) & (index < until)
        a_list, a_ends = by_piece(a_place, here, wanted, index)
        b_list, b_ends = by_piece(b_place, here, wanted, index)
        head = jnp.arange(16, dtype=jnp.int32)
        span = jnp.where(head == 0, begin, until)
        plans.append(jnp.concatenate([span, a_ends, b_ends, image_at, a_list, b_list, depth]))
    return group, plans


def body(images, slices, classes, rotations, defocus, groups):
    core = lax.axis_index("c")
    facts = jnp.stack([classes, rotations, defocus, groups])
    facts = jnp.concatenate([facts, swapped(facts)], 1)
    own = by_rows(images)
    other = swapped(own)
    own_slices = by_rows(slices[0])
    slices_a = gather_part(own_slices[:, :ROWS_A], RINGS_A)
    slices_b = gather_part(own_slices[:, ROWS_A:], RINGS_B)
    group, plans = plan(facts, core)
    sums = None
    for held, one in (((EARLY, EARLY), plans[0]), ((ALL, ALL), plans[1])):
        sums = shell_sums(held, one, sums, own, other, slices_a, slices_b)
    lane = jnp.arange(128, dtype=jnp.int32)
    inner = jnp.pad(sums[:, : SHELLS - 1], ((0, 0), (1, 128 - SHELLS)))
    sums = jnp.where(lane < SHELLS, sums - inner, jnp.where(lane == SHELLS, 1.0, 0.0))
    high = lax.reduce_precision(sums, 8, 7)
    parts = jnp.concatenate([high, sums - high], 1).astype(jnp.bfloat16)
    member = (jnp.arange(GROUPS, dtype=jnp.int32)[:, None] == group[None, :]).astype(jnp.bfloat16)
    partial = jnp.dot(member, parts, preferred_element_type=jnp.float32)
    partial = partial[:, :128] + partial[:, 128:]
    partial = partial[:, :COLUMNS].reshape(DEVICES, GROUPS_DEV * COLUMNS)
    arrived = lax.all_to_all(partial, AXES, 0, 0, tiled=True)
    own_groups = jnp.sum(arrived, axis=0).reshape(GROUPS_DEV, COLUMNS)
    return own_groups[:, :SHELLS] / (2.0 * own_groups[:, SHELLS : SHELLS + 1] * jnp.asarray(shell_pixels()))


def solution(mesh):
    finer = Mesh(mesh.devices.reshape(4, 4, 4, 2), AXES)
    placed = (
        P(AXES, None, None),
        P(AXES, None, None, None),
        P(AXES),
        P(AXES),
        P(AXES),
        P(AXES),
    )
    return jax.shard_map(body, mesh=finer, in_specs=placed, out_specs=P(AXES, None), check_vma=False)
```

```python
import functools
import math

import jax
import jax.numpy as jnp
import numpy as np
from jax import lax
from jax.experimental import pallas as pl
from jax.experimental.pallas import tpu as pltpu
from jax.sharding import Mesh
from jax.sharding import PartitionSpec as P


AXES = ("z", "y", "x", "c")
RING = 4
SIDE = 128
HALF = SIDE // 2
SHELLS = 64
ROT = 4
P_DEV = 128
GROUPS_DEV = 8
DEVICES = 128
GROUPS = GROUPS_DEV * DEVICES
CANDIDATES = 2 * P_DEV

PIXEL_SIZE = 1.5
WAVELENGTH = 0.0197
SPHERICAL = 27000000.0
AMPLITUDE = 0.1

ROWS = 2 * SIDE
ROWS_A = 176
ROWS_B = ROWS - ROWS_A
RINGS_A = (("y", "z", "x"), ("x", "y", "z"))
RINGS_B = (("x", "z", "y"), ("z", "x", "y"))

DEPTH = 32
PACK = 4
STEP = 2 * PACK
RESULTS = CANDIDATES + STEP
A_ENDS, B_ENDS, IMAGE_AT = 16, 32, 48
A_LIST, B_LIST, DEPTH_AT = IMAGE_AT + RESULTS, IMAGE_AT + 2 * RESULTS, IMAGE_AT + 3 * RESULTS
LENGTHS = (16, 16, 16, 8, 8) + 3 * (16, 32, 16)
ALL = tuple(range(len(LENGTHS)))
EARLY = tuple(b for b in ALL if b not in (8, 9, 10))
SPAN = 64
NOWHERE = 127
COLUMNS = 80


def sine_terms():
    turns = np.cos(np.linspace(0, np.pi, 4001)) * 0.5
    turns = turns[np.abs(turns) > 1e-9]
    basis = np.stack([np.abs(turns) * turns ** (2 * k) for k in range(6)], 1)
    target = np.sin(2 * np.pi * turns) / turns * np.abs(turns)
    return [float(c) for c in np.linalg.lstsq(basis, target, rcond=None)[0]]


SINE = sine_terms()


def frequencies():
    offsets = np.arange(SIDE)
    return np.where(offsets < SIDE // 2, offsets, offsets - SIDE)


def tables():
    freq = frequencies()
    radius_sq = (freq[:, None] ** 2 + freq[None, :] ** 2).astype(np.float64)
    spatial = radius_sq / (SIDE * PIXEL_SIZE) ** 2
    rate = 0.5 * WAVELENGTH * spatial
    shift = -0.25 * SPHERICAL * WAVELENGTH**3 * spatial**2 + math.asin(AMPLITUDE) / (2 * math.pi)
    within = np.zeros((SIDE, 128), np.float32)
    for w in range(SIDE // 2 + 1):
        within[:, w] = np.abs(freq) <= w
    reach = np.full((HALF + 8, 128), NOWHERE, np.int32)
    for a in range(HALF + 1):
        for s in range(SHELLS):
            left = (s + 1) ** 2 - 1 - int(freq[a]) ** 2
            if left >= 0:
                reach[a, s] = min(math.isqrt(left), SIDE // 2)
    half = HALF + 8
    return (
        rate[:half].astype(np.float32),
        shift[:half].astype(np.float32),
        np.concatenate([within, within], 0),
        reach,
    )


def shell_pixels():
    freq = frequencies()
    radius_sq = freq[:, None] ** 2 + freq[None, :] ** 2
    return np.array(
        [((s * s <= radius_sq) & (radius_sq < (s + 1) ** 2)).sum() for s in range(SHELLS)], np.float32
    )


def shell_kernel(
    plan_ref, *refs, held, first,
):
    done, refs = (None, refs) if first else (refs[0], refs[1:])
    own, other, *refs = refs
    pieces = len(held[0]) + len(held[1])
    slices_a, slices_b = refs[: len(held[0])], refs[len(held[0]) : pieces]
    constants, (out, *scratch) = refs[pieces : pieces + 4], refs[pieces + 4 :]
    tables_here, (image, fetched, square, terms, image_sem, slice_sem, table_sem) = scratch[:4], scratch[4:]
    rate, shift, within, reach = tables_here
    begin, total = plan_ref[0], plan_ref[1]

    def table_copies():
        return [
            pltpu.make_async_copy(there, here, table_sem.at[i])
            for i, (there, here) in enumerate(zip(constants, tables_here))
        ]

    def fetch_slices(places, ends, numbers, parts, rows):
        for b, part in zip(numbers, parts):
            low, high = plan_ref[ends + b], plan_ref[ends + b + 1]

            def fetch(t, part=part):
                entry = plan_ref[places + t]
                j, at = entry // SPAN, entry % SPAN
                pltpu.make_async_copy(part.at[at], fetched.at[j, rows], slice_sem.at[j // STEP]).start()

            def fetch_some(i, carry, fetch=fetch, low=low):
                for k in range(4):
                    fetch(low + 4 * i + k)
                return carry

            fours = (high - low) // 4
            lax.fori_loop(0, fours, fetch_some, 0)
            for k in range(3):
                left_over = low + 4 * fours + k

                @pl.when(left_over < high)
                def _(fetch=fetch, left_over=left_over):
                    fetch(left_over)

    def start(j, slot):
        at = plan_ref[IMAGE_AT + j]

        @pl.when(at < P_DEV)
        def _():
            pltpu.make_async_copy(own.at[at], image.at[slot], image_sem.at[slot]).start()

        @pl.when(at >= P_DEV)
        def _():
            pltpu.make_async_copy(other.at[at - P_DEV], image.at[slot], image_sem.at[slot]).start()

    def wait(slot):
        pltpu.make_async_copy(own.at[0], image.at[slot], image_sem.at[slot]).wait()

    for copy in table_copies():
        copy.start()

    def start_early(j, carry):
        start(j, lax.rem(j, DEPTH))
        return carry

    lax.fori_loop(begin, jnp.minimum(begin + DEPTH, total), start_early, 0)
    fetch_slices(A_LIST, A_ENDS, held[0], slices_a, pl.ds(0, ROWS_A))
    fetch_slices(B_LIST, B_ENDS, held[1], slices_b, pl.ds(ROWS_A, ROWS_B))
    sublane = lax.broadcasted_iota(jnp.int32, (8, 128), 0)
    out[...] = jnp.zeros_like(out) if first else done[...]
    half, top = sublane // 2, sublane == 0
    back = jnp.where(top, 0, 8 - sublane)
    first = half == 0
    low, high, zero, down = half, half + 4, half * 0, 4 - half
    wrap = jnp.where(first, 0, 8 - half)

    def rows_of(v, index):
        return jnp.take_along_axis(v, index, axis=0, mode="promise_in_bounds")

    def waves(j):
        depth = plan_ref[DEPTH_AT + j].astype(jnp.float32)
        result = []
        for g in range(SIDE // 16 + 1):
            turns = depth * rate[8 * g : 8 * g + 8, :] + shift[8 * g : 8 * g + 8, :]
            turns = turns - jnp.round(turns)
            sq = turns * turns
            y = sq * SINE[-1] + SINE[-2]
            for term in SINE[-3::-1]:
                y = y * sq + term
            result.append(y * turns)
        return result

    def spread(s, v):
        if v < 16:
            return rows_of(s[v // 2], high if v % 2 else low)
        h = v - 16
        if h % 2:
            return rows_of(s[(15 - h) // 2], down)
        m = 8 - h // 2
        return jnp.where(first, rows_of(s[m], zero), rows_of(s[m - 1], wrap))

    def keep(k, at, pair):
        p = jnp.concatenate(pair, 0)
        high_part = p.astype(jnp.bfloat16)
        terms[k, at : at + 16, 0:128] = high_part
        terms[k, at : at + 16, 128:256] = (p - high_part.astype(jnp.float32)).astype(jnp.bfloat16)

    def power(j, slot, k, m):
        s = waves(j)

        def pixel_power(g):
            for h in range(2):
                v = 4 * g + 2 * h
                r = pl.ds(8 * v, 16)
                wave = jnp.concatenate([spread(s, v), spread(s, v + 1)], 0)
                e = image[slot, r, :].astype(jnp.float32) + wave * fetched[j, r, :].astype(jnp.float32)
                square[m % 2, r, :] = e * e
            both = [square[m % 2, pl.ds(32 * g + part, 16, stride=2), :] for part in range(2)]
            p = both[0] + both[1]
            return [p[:8], p[8:]]

        turned = [rows_of(p, back) for g in range(4, 8) for p in pixel_power(g)]
        turned.append(jnp.zeros((8, 128), jnp.float32))
        for g in range(4):
            near = pixel_power(g)
            for h in range(2):
                v = 2 * g + h
                near[h] = near[h] + jnp.where(top, turned[8 - v], turned[7 - v])
            keep(k, HALF * m + 16 * g, near)
        return jnp.where(top, turned[0], 0.0)

    def keep_edges(edges, k):
        for at in range(0, PACK, 2):
            keep(k, HALF * PACK + 8 * at, edges[at : at + 2])

    def collect(sums, j, m):
        parts = [jnp.zeros((8, 128), jnp.float32) for _ in range(2)]
        starts = [HALF * m + 8 * g for g in range(8)] + [HALF * PACK + 8 * m]
        for g, at in enumerate(starts):
            index = reach[8 * g : 8 * g + 8, :]
            found = jnp.take_along_axis(sums[at : at + 8], index, axis=1, mode="promise_in_bounds")
            parts[g % 2] = parts[g % 2] + found
        out[pl.ds(j, 1), :] = jnp.sum(parts[0] + parts[1], axis=0, keepdims=True)

    def region(j, slot, k, before):
        sums = jnp.dot(terms[1 - k], within[...], preferred_element_type=jnp.float32)
        edges = []
        for m in range(PACK):
            edges.append(power(j + m, slot + m, k, m))
            collect(sums, before + m, m)
        keep_edges(edges, k)

    def step(i, carry):
        j = STEP * i
        slot = lax.rem(j, DEPTH)
        block = fetched.at[pl.ds(j, STEP)]
        pltpu.make_async_copy(own.at[pl.ds(0, STEP)], block, slice_sem.at[i]).wait()
        for m in range(STEP):
            wait(slot + m)
        region(j, slot, 0, jnp.maximum(j - PACK, begin))
        region(j + PACK, slot + PACK, 1, j)
        for m in range(STEP):

            @pl.when(j + m + DEPTH < total)
            def _(m=m):
                start(j + m + DEPTH, slot + m)

        return carry

    terms[...] = jnp.zeros_like(terms)
    for copy in table_copies():
        copy.wait()
    lax.fori_loop(begin // STEP, total // STEP, step, 0)

    @pl.when(total > begin)
    def _():
        sums = jnp.dot(terms[1], within[...], preferred_element_type=jnp.float32)
        for m in range(PACK):
            collect(sums, total - PACK + m, m)


def shell_sums(held, plan, done, own, other, slices_a, slices_b):
    before = () if done is None else (done,)
    rate, shift, within, reach = tables()
    constants = jnp.asarray(rate), jnp.asarray(shift), jnp.asarray(within, jnp.bfloat16), jnp.asarray(reach)
    smem = pl.BlockSpec(memory_space=pltpu.SMEM)
    hbm = pl.BlockSpec(memory_space=pltpu.HBM)
    vmem = pl.BlockSpec(memory_space=pltpu.VMEM)
    return pl.pallas_call(
        functools.partial(shell_kernel, held=held, first=done is None),
        out_shape=jax.ShapeDtypeStruct((RESULTS, 128), jnp.float32),
        in_specs=[smem] + [vmem] * len(before) + [hbm] * (2 + len(held[0]) + len(held[1]) + len(constants)),
        out_specs=vmem,
        scratch_shapes=[
            *(pltpu.VMEM(c.shape, c.dtype) for c in constants),
            pltpu.VMEM((DEPTH, ROWS, 128), jnp.bfloat16),
            pltpu.VMEM((RESULTS, ROWS, 128), jnp.bfloat16),
            pltpu.VMEM((2, ROWS, 128), jnp.float32),
            pltpu.VMEM((2, (HALF + 8) * PACK, 256), jnp.bfloat16),
            pltpu.SemaphoreType.DMA((DEPTH,)),
            pltpu.SemaphoreType.DMA((RESULTS // STEP,)),
            pltpu.SemaphoreType.DMA((len(constants),)),
        ],
    )(
        plan, *before, own, other,
        *(slices_a[b] for b in held[0]), *(slices_b[b] for b in held[1]), *constants,
    )


def ring_pairs(rings, step):
    pairs = []
    for source in range(DEVICES):
        at = {"z": source // 32, "y": source // 8 % 4, "x": source // 2 % 4, "c": source % 2}
        to = dict(at)
        ring = rings[at["c"]]
        to[ring] = (at[ring] + step) % RING
        pairs.append((source, ((to["z"] * 4 + to["y"]) * 4 + to["x"]) * 2 + to["c"]))
    return pairs


def send(x, rings, step):
    return lax.ppermute(x, AXES, ring_pairs(rings, step))


def joined(parts):
    return jnp.concatenate(parts, 0)


def last_ring(own, near, rest, rings):
    parts = own, near, rest
    left = [send(x, rings, 1) for x in parts]
    right = [send(x, rings, -1) for x in parts]
    far = (send(right[0], rings, -1), send(left[1], rings, 1), send(right[2], rings, -1))
    return (*right, *far, *left)


def gather_part(x, rings):
    first, second, third = zip(*rings)
    x = x, send(x, first, -1), send(x, first, 2), send(x, first, 1)
    block = joined(x)
    half = block.shape[0] // 2
    right, left = send(block, second, -1), send(block, second, 1)
    far = send(left[:half], second, 1), send(right[half:], second, -1)
    near, rest = joined((right, left)), joined(far)
    return (block, right, left, *far, *last_ring(block, near, rest, third))


def place_of(owner, rotation, rings, core):
    here = {a: lax.axis_index(a) for a in AXES}
    ahead = {
        "z": (owner // 32 - here["z"]) % RING,
        "y": (owner // 8 % 4 - here["y"]) % RING,
        "x": (owner // 2 % 4 - here["x"]) % RING,
    }
    places = [
        ((ahead[r[2]] * 4 + (ahead[r[1]] ^ (ahead[r[1]] >> 1))) * 4 + ahead[r[0]]) * ROT + rotation for r in rings
    ]
    return jnp.where(core == 0, places[0], places[1])


def by_piece(place, here, wanted, index):
    starts = np.cumsum((0,) + LENGTHS)
    place = jnp.where(here, place, 0)
    piece = sum((place >= int(edge)).astype(jnp.int32) for edge in starts[1:-1])
    at = place - sum(jnp.where(piece == b, int(starts[b]), 0) for b in range(len(LENGTHS)))
    piece = jnp.where(wanted, piece, len(LENGTHS))
    key = piece * RESULTS + index
    rank = jnp.sum((key[None, :] < key[:, None]).astype(jnp.int32), axis=1)
    entry = index * SPAN + at
    places = jnp.sum(jnp.where(rank[None, :] == index[:, None], entry[None, :], 0), axis=1)
    edges = jnp.arange(16, dtype=jnp.int32)
    return places, jnp.sum((piece[None, :] < edges[:, None]).astype(jnp.int32), axis=1)


def swapped(x):
    return lax.ppermute(x, "c", [(0, 1), (1, 0)])


def by_rows(x):
    lead = x.shape[:-2]
    x = x.reshape(*lead, 2, SIDE, SIDE)
    return jnp.swapaxes(x, -3, -2).reshape(*lead, ROWS, SIDE)


def plan(facts, core):
    owner, rotation, depth, group = facts
    mine = owner % 2 == core
    a_place = place_of(owner, rotation, RINGS_A, core)
    b_place = place_of(owner, rotation, RINGS_B, core)
    late = mine & ((a_place // SPAN == 2) | (b_place // SPAN == 2))
    early = mine & ~late

    def ranks(mask):
        i = jnp.arange(CANDIDATES, dtype=jnp.int32)
        before = (i[None, :] < i[:, None]) & mask[None, :]
        return jnp.sum(before.astype(jnp.int32), axis=1), jnp.sum(mask.astype(jnp.int32))

    def whole_steps(n):
        return (n + STEP - 1) // STEP * STEP

    early_rank, early_count = ranks(early)
    late_rank, late_count = ranks(late)
    middle = whole_steps(early_count)
    end = middle + whole_steps(late_count)
    index = jnp.arange(RESULTS, dtype=jnp.int32)
    row = jnp.where(early, early_rank, jnp.where(late, middle + late_rank, -1))
    chosen = row[None, :] == index[:, None]

    def packed(values):
        return jnp.sum(jnp.where(chosen, values[None, :], 0), axis=1)

    depth = packed(depth)
    here = (index < early_count) | ((index >= middle) & (index < middle + late_count))
    group = jnp.where(here, packed(group), -1)
    image_at = packed(jnp.arange(CANDIDATES, dtype=jnp.int32))
    a_place, b_place = packed(a_place), packed(b_place)
    plans = []
    for begin, until in ((jnp.int32(0), middle), (middle, end)):
        wanted = (index >= begin) & (index < until)
        a_list, a_ends = by_piece(a_place, here, wanted, index)
        b_list, b_ends = by_piece(b_place, here, wanted, index)
        head = jnp.arange(16, dtype=jnp.int32)
        span = jnp.where(head == 0, begin, until)
        plans.append(jnp.concatenate([span, a_ends, b_ends, image_at, a_list, b_list, depth]))
    return group, plans


def body(images, slices, classes, rotations, defocus, groups):
    core = lax.axis_index("c")
    facts = jnp.stack([classes, rotations, defocus, groups])
    facts = jnp.concatenate([facts, swapped(facts)], 1)
    own = by_rows(images)
    other = swapped(own)
    own_slices = by_rows(slices[0])
    slices_a = gather_part(own_slices[:, :ROWS_A], RINGS_A)
    slices_b = gather_part(own_slices[:, ROWS_A:], RINGS_B)
    group, plans = plan(facts, core)
    sums = None
    for held, one in (((EARLY, EARLY), plans[0]), ((ALL, ALL), plans[1])):
        sums = shell_sums(held, one, sums, own, other, slices_a, slices_b)
    lane = jnp.arange(128, dtype=jnp.int32)
    inner = jnp.pad(sums[:, : SHELLS - 1], ((0, 0), (1, 128 - SHELLS)))
    sums = jnp.where(lane < SHELLS, sums - inner, jnp.where(lane == SHELLS, 1.0, 0.0))
    high = lax.reduce_precision(sums, 8, 7)
    parts = jnp.concatenate([high, sums - high], 1).astype(jnp.bfloat16)
    member = (jnp.arange(GROUPS, dtype=jnp.int32)[:, None] == group[None, :]).astype(jnp.bfloat16)
    partial = jnp.dot(member, parts, preferred_element_type=jnp.float32)
    partial = partial[:, :128] + partial[:, 128:]
    partial = partial[:, :COLUMNS].reshape(DEVICES, GROUPS_DEV * COLUMNS)
    arrived = lax.all_to_all(partial, AXES, 0, 0, tiled=True)
    own_groups = jnp.sum(arrived, axis=0).reshape(GROUPS_DEV, COLUMNS)
    return own_groups[:, :SHELLS] / (2.0 * own_groups[:, SHELLS : SHELLS + 1] * jnp.asarray(shell_pixels()))


def solution(mesh):
    finer = Mesh(mesh.devices.reshape(4, 4, 4, 2), AXES)
    placed = (
        P(AXES, None, None),
        P(AXES, None, None, None),
        P(AXES),
        P(AXES),
        P(AXES),
        P(AXES),
    )
    return jax.shard_map(body, mesh=finer, in_specs=placed, out_specs=P(AXES, None), check_vma=False)
```
